8 devices in a mesh: dp: 1 (over z), sp: 8 (over x, y, core).
Axes of the slice: x: 2, y: 2, z: 1, core: 2. Of those that a mesh axis runs over, the one named last changes fastest.
Arguments:
- q: bfloat16 [32, 32, 64], P('dp')
- k: bfloat16 [32, 4096, 32, 64], P('dp', 'sp')
- v: bfloat16 [32, 4096, 32, 64], P('dp', 'sp')
Outputs:
- q: bfloat16 [32, 32, 64], P('dp')
All inputs are finite; a program needn't handle non-finite values.
Results may differ from the reference program's by a relative error of at most 0.012.
Values are sent between devices in bfloat16 or wider.
A program may use at most 2 GiB of HBM per device.

```python
import jax
import jax.numpy as jnp

BATCH = 32
CACHE = 4096
HEADS = 32
KV_HEADS = 32
HEAD = 64


def setup_inputs(seed: int = 0, part: int = 0) -> dict:
    kq, kk, kv = (jax.random.fold_in(k, part) for k in jax.random.split(jax.random.key(seed), 3))
    return {
        "q": (3 * jax.random.normal(kq, (BATCH, HEADS, HEAD), jnp.float32)).astype(jnp.bfloat16),
        "k": jax.random.normal(kk, (BATCH, CACHE, KV_HEADS, HEAD), jnp.float32).astype(jnp.bfloat16),
        "v": jax.random.normal(kv, (BATCH, CACHE, KV_HEADS, HEAD), jnp.float32).astype(jnp.bfloat16),
    }


def einsum(form, a, b):
    return jnp.einsum(form, a.astype(jnp.float32), b.astype(jnp.float32))


def reference(q, k, v):
    grouped = q.reshape(BATCH, KV_HEADS, -1, HEAD)
    scores = einsum("bgsd,bugd->bgsu", grouped, k) * HEAD**-0.5
    weights = jax.nn.softmax(scores, -1).astype(jnp.bfloat16)
    return einsum("bgsu,bugd->bgsd", weights, v).astype(jnp.bfloat16).reshape(BATCH, HEADS, HEAD)
```

```python
import functools

import jax
import jax.numpy as jnp
from jax import lax
from jax.experimental import pallas as pl
from jax.experimental.pallas import tpu as pltpu
from jax.sharding import PartitionSpec as P

MESH = pl.DeviceIdType.MESH
SLOTS = 6
LAG = 4
GROUP = 8
PEERS = [(x, y, c) for x in (1, 0) for y in (1, 0) for c in (1, 0)][:-1]


def attend(pairs, heads, head, q_hbm, k_hbm, v_hbm, out_ref, q_ref, kbuf, vbuf, weights, part, stat, parts, stats, qsem, ksem, vsem, send, recv):
    batch, groups, lanes = 2 * pairs, heads // GROUP, 2 * head
    tokens = kbuf.shape[2]
    me = lax.axis_index("sp")
    mx, my, mc = me // 4, (me // 2) % 2, me % 2
    devices = [((mx + x) % 2) * 4 + ((my + y) % 2) * 2 + (mc + c) % 2 for x, y, c in PEERS]

    def kcopy(b):
        return pltpu.make_async_copy(k_hbm.at[b], kbuf.at[b % SLOTS], ksem.at[b % SLOTS])

    def vcopy(b):
        return pltpu.make_async_copy(v_hbm.at[b], vbuf.at[b % SLOTS], vsem.at[b % SLOTS])

    qcopy = pltpu.make_async_copy(q_hbm, q_ref, qsem)
    qcopy.start()
    for b in range(SLOTS):
        kcopy(b).start()
        if b:
            vcopy(b - 1).start()
    vcopy(SLOTS - 1).start()

    barrier = pltpu.get_barrier_semaphore()
    for device in devices:
        pl.semaphore_signal(barrier, inc=1, device_id={"sp": device}, device_id_type=MESH)

    lane = lax.broadcasted_iota(jnp.int32, (GROUP, 2 * head), 1)
    row = lax.broadcasted_iota(jnp.int32, (GROUP, 2 * head), 0)
    own = [row == 2 * j + lane // head for j in range(GROUP // 2)]
    first = lane < head

    def scores(b, stat_tile):
        kcopy(b).wait()
        queries = q_ref[b].astype(jnp.float32)
        for g in range(groups):
            query = queries[g * GROUP : (g + 1) * GROUP]
            query = jnp.concatenate([query, query], 1)
            spread = jnp.concatenate([jnp.where(o, query, 0.0) for o in own], 1).astype(jnp.bfloat16)
            keys = kbuf[b % SLOTS, g * GROUP * head : (g + 1) * GROUP * head, :]
            s = jnp.dot(spread, keys, preferred_element_type=jnp.float32) * head**-0.5
            high = jnp.max(s, 1, keepdims=True)
            w = jnp.exp(s - high)
            weights[b % 2, g * GROUP : (g + 1) * GROUP, :] = w
            total = jnp.sum(w, 1, keepdims=True)
            at = g * 4 + (b % 2) * 2
            stat_tile = jnp.where(lane == at, high, jnp.where(lane == at + 1, total, stat_tile))
        return stat_tile

    def values(b):
        vcopy(b).wait()
        tiles = []
        for g in range(groups):
            w = weights[b % 2, g * GROUP : (g + 1) * GROUP, :].astype(jnp.bfloat16)
            block = vbuf[b % SLOTS, g * GROUP * head : (g + 1) * GROUP * head, :]
            seen = lax.dot_general(w, block, (((1,), (1,)), ((), ())), preferred_element_type=jnp.float32)
            folded = sum(jnp.where(o, seen[:, j * lanes : (j + 1) * lanes], 0.0) for j, o in enumerate(own))
            tiles.append(folded + pltpu.roll(folded, head, 1))
        return tiles

    def copies(p, kind):
        src, dst = ((part, parts), (stat, stats))[kind]
        return [
            pltpu.make_async_remote_copy(
                src_ref=src.at[p],
                dst_ref=dst.at[r, p],
                send_sem=send.at[p % 2, r, kind],
                recv_sem=recv.at[p, r, kind],
                device_id={"sp": device},
                device_id_type=MESH,
            )
            for r, device in enumerate(devices)
        ]

    def together(p):
        for copy in copies(p, 0) + copies(p, 1):
            copy.wait_recv()
        each = [stat[p]] + [stats[r, p] for r in range(len(PEERS))]
        high = functools.reduce(jnp.maximum, each)
        scale = [jnp.exp(e - high) for e in each]
        total = sum(pltpu.roll(e, 2 * head - 1, 1) * s for e, s in zip(each, scale))
        scale = [s / total for s in scale]
        result = [[], []]
        for h in range(groups // 2):
            tiles = [part[p, h * 2 * GROUP : (h + 1) * 2 * GROUP, :]] + [parts[r, p, h * 2 * GROUP : (h + 1) * 2 * GROUP, :] for r in range(len(PEERS))]
            tiles = [t.astype(jnp.float32) for t in tiles]
            both = []
            for i in range(2):
                g = 2 * h + i
                both.append(
                    sum(
                        t[i * GROUP : (i + 1) * GROUP] * jnp.where(first, s[:, 4 * g : 4 * g + 1], s[:, 4 * g + 2 : 4 * g + 3])
                        for t, s in zip(tiles, scale)
                    )
                )
            both = jnp.concatenate(both, 0)
            result[0].append(both[:, :head])
            result[1].append(pltpu.roll(both, head, 1)[:, :head])
        for i in range(2):
            out_ref[2 * p + i] = jnp.concatenate(result[i], 0).astype(out_ref.dtype)

    def refill(copy, b):
        @pl.when(b + SLOTS < batch)
        def _():
            copy(b + SLOTS).start()

    qcopy.wait()
    stat[0] = scores(0, jnp.zeros((GROUP, lanes), jnp.float32))
    refill(kcopy, 0)

    def pair(p, last):
        b = 2 * p
        even = values(b)
        stat[p] = scores(b + 1, stat[p])
        refill(vcopy, b)
        refill(kcopy, b + 1)
        if last:
            for copy in copies(p, 1):
                copy.start()
        odd = values(b + 1)
        for h in range(groups // 2):
            tile = jnp.concatenate([jnp.where(first, even[g], odd[g]) for g in (2 * h, 2 * h + 1)], 0)
            part[p, h * 2 * GROUP : (h + 1) * 2 * GROUP, :] = tile.astype(part.dtype)
        if last:
            for copy in copies(p, 0):
                copy.start()
        else:
            stat[p + 1] = scores(b + 2, jnp.zeros((GROUP, lanes), jnp.float32))
            refill(vcopy, b + 1)
            refill(kcopy, b + 2)

    def send_pair(p):
        for copy in copies(p, 0) + copies(p, 1):
            copy.start()

    def sent(p):
        for copy in copies(p, 0) + copies(p, 1):
            copy.wait_send()

    pair(0, False)
    pl.semaphore_wait(barrier, len(PEERS))

    @pl.loop(1, pairs - 1)
    def _(p):
        @pl.when(p >= 3)
        def _():
            sent(p - 3)

        send_pair(p - 1)
        pair(p, False)

        @pl.when(p >= LAG)
        def _():
            together(p - LAG)

    p = pairs - 1
    sent(p - 3)
    send_pair(p - 1)
    sent(p - 2)
    pair(p, True)

    @pl.loop(p - LAG, pairs)
    def _(c):
        together(c)

    sent(p - 1)
    sent(p)


def solution(mesh):
    def step(q, k, v):
        batch, tokens, heads, head = k.shape
        pairs = batch // 2
        k, v = (jnp.transpose(x, (0, 2, 3, 1)).reshape(batch, heads * head, tokens) for x in (k, v))
        n = len(PEERS)
        block = pltpu.VMEM((SLOTS, heads * head, tokens), jnp.bfloat16)
        return pl.pallas_call(
            functools.partial(attend, pairs, heads, head),
            out_shape=jax.ShapeDtypeStruct(q.shape, q.dtype),
            in_specs=[pl.BlockSpec(memory_space=pl.ANY)] * 3,
            out_specs=pl.BlockSpec(memory_space=pltpu.VMEM),
            scratch_shapes=[
                pltpu.VMEM(q.shape, q.dtype),
                block,
                block,
                pltpu.VMEM((2, heads, tokens), jnp.float32),
                pltpu.VMEM((pairs, heads, 2 * head), jnp.bfloat16),
                pltpu.VMEM((pairs, GROUP, 2 * head), jnp.float32),
                pltpu.VMEM((n, pairs, heads, 2 * head), jnp.bfloat16),
                pltpu.VMEM((n, pairs, GROUP, 2 * head), jnp.float32),
                pltpu.SemaphoreType.DMA,
                pltpu.SemaphoreType.DMA((SLOTS,)),
                pltpu.SemaphoreType.DMA((SLOTS,)),
                pltpu.SemaphoreType.DMA((2, n, 2)),
                pltpu.SemaphoreType.DMA((pairs, n, 2)),
            ],
            compiler_params=pltpu.CompilerParams(collective_id=0, has_side_effects=True, vmem_limit_bytes=48 * 2**20),
        )(q, k, v)

    return jax.shard_map(
        step,
        mesh=mesh,
        in_specs=(P("dp", None, None), P("dp", "sp", None, None), P("dp", "sp", None, None)),
        out_specs=P("dp", None, None),
        check_vma=False,
    )
```

```python
import functools

import jax
import jax.numpy as jnp
from jax import lax
from jax.experimental import pallas as pl
from jax.experimental.pallas import tpu as pltpu
from jax.sharding import PartitionSpec as P

MESH = pl.DeviceIdType.MESH
SLOTS = 6
LAG = 4
GROUP = 8
PEERS = [(x, y, c) for x in (1, 0) for y in (1, 0) for c in (1, 0)][:-1]


def add(terms):
    return functools.reduce(jnp.add, terms)


def attend(pairs, heads, head, q_hbm, k_hbm, v_hbm, out_ref, q_ref, kbuf, vbuf, weights, part, stat, parts, stats, qsem, ksem, vsem, lsem, send, recv):
    batch, groups, lanes = 2 * pairs, heads // GROUP, 2 * head
    rows = GROUP * head
    me = lax.axis_index("sp")
    mx, my, mc = me // 4, (me // 2) % 2, me % 2
    devices = [((mx + x) % 2) * 4 + ((my + y) % 2) * 2 + (mc + c) % 2 for x, y, c in PEERS]

    def kcopy(b):
        return pltpu.make_async_copy(k_hbm.at[b], kbuf.at[b % SLOTS], ksem.at[b % SLOTS])

    def vcopy(b):
        return pltpu.make_async_copy(v_hbm.at[b], vbuf.at[b % SLOTS], vsem.at[b % SLOTS])

    def vpiece(b, g):
        piece = pl.ds(g * rows, rows)
        return pltpu.make_async_copy(v_hbm.at[b, piece], vbuf.at[b % SLOTS, piece], lsem.at[b % 2, g])

    qcopy = pltpu.make_async_copy(q_hbm, q_ref, qsem)
    qcopy.start()
    kcopy(0).start()
    kcopy(1).start()
    for b in range(SLOTS - 2):
        kcopy(b + 2).start()
        vcopy(b).start()

    barrier = pltpu.get_barrier_semaphore()
    for device in devices:
        pl.semaphore_signal(barrier, inc=1, device_id={"sp": device}, device_id_type=MESH)

    lane = lax.broadcasted_iota(jnp.int32, (GROUP, lanes), 1)
    row = lax.broadcasted_iota(jnp.int32, (GROUP, lanes), 0)
    own = [row == 2 * j + lane // head for j in range(GROUP // 2)]
    odd = (lane // head) == row % 2

    def scores(b, i, stat_tile):
        queries = q_ref[b].astype(jnp.float32)
        for g in range(groups):
            query = queries[g * GROUP : (g + 1) * GROUP]
            query = jnp.concatenate([query, query], 1)
            spread = jnp.concatenate([jnp.where(o, query, 0.0) for o in own], 1).astype(jnp.bfloat16)
            keys = kbuf[b % SLOTS, g * rows : (g + 1) * rows, :]
            s = jnp.dot(spread, keys, preferred_element_type=jnp.float32) * head**-0.5
            high = jnp.max(s, 1, keepdims=True)
            w = jnp.exp(s - high)
            weights[i, g * GROUP : (g + 1) * GROUP, :] = w
            total = jnp.sum(w, 1, keepdims=True)
            at = g * 4 + i * 2
            stat_tile = jnp.where(lane == at, high, jnp.where(lane == at + 1, total, stat_tile))
        return stat_tile

    def values(b, i, g):
        w = weights[i, g * GROUP : (g + 1) * GROUP, :].astype(jnp.bfloat16)
        block = vbuf[b % SLOTS, g * rows : (g + 1) * rows, :]
        seen = lax.dot_general(w, block, (((1,), (1,)), ((), ())), preferred_element_type=jnp.float32)
        return add(jnp.where(o, seen[:, j * lanes : (j + 1) * lanes], 0.0) for j, o in enumerate(own))

    def stat_copies(p):
        return [
            pltpu.make_async_remote_copy(
                src_ref=stat.at[p],
                dst_ref=stats.at[r, p],
                send_sem=send.at[p % 2, r, 0],
                recv_sem=recv.at[p, r, 0],
                device_id={"sp": device},
                device_id_type=MESH,
            )
            for r, device in enumerate(devices)
        ]

    def part_copies(p, at=0, size=heads, sem=1):
        piece = pl.ds(at, size)
        return [
            pltpu.make_async_remote_copy(
                src_ref=part.at[p, piece],
                dst_ref=parts.at[r, p, piece],
                send_sem=send.at[p % 2, r, sem],
                recv_sem=recv.at[p, r, sem],
                device_id={"sp": device},
                device_id_type=MESH,
            )
            for r, device in enumerate(devices)
        ]

    def half_copies(p, h):
        return part_copies(p, h * 2 * GROUP, 2 * GROUP, 1 + h)

    def scales(p):
        each = [stat[p]] + [stats[r, p] for r in range(len(PEERS))]
        high = functools.reduce(jnp.maximum, each)
        scale = [jnp.exp(e - high) for e in each]
        total = add(pltpu.roll(e, lanes - 1, 1) * s for e, s in zip(each, scale))
        scale = [s / total for s in scale]
        return [[jnp.where(odd, s[:, 4 * g + 2 : 4 * g + 3], s[:, 4 * g : 4 * g + 1]) for s in scale] for g in range(groups)]

    def together(p, h, scale):
        piece = slice(h * 2 * GROUP, (h + 1) * 2 * GROUP)
        tiles = [t.astype(jnp.float32) for t in [part[p, piece, :]] + [parts[r, p, piece, :] for r in range(len(PEERS))]]
        result = [[], []]
        for i in range(2):
            both = add(t[i * GROUP : (i + 1) * GROUP] * s for t, s in zip(tiles, scale[2 * h + i]))
            swapped = pltpu.roll(both, head, 1)
            result[0].append(jnp.where(row % 2 == 0, swapped, both)[:, :head])
            result[1].append(jnp.where(row % 2 == 0, both, swapped)[:, :head])
        for i in range(2):
            out_ref[2 * p + i, piece, :] = jnp.concatenate(result[i], 0).astype(out_ref.dtype)

    def store(p, even, odd_tiles, h):
        tile = jnp.concatenate([pltpu.roll(even[g], head, 1) + odd_tiles[g] for g in (2 * h, 2 * h + 1)], 0)
        part[p, h * 2 * GROUP : (h + 1) * 2 * GROUP, :] = tile.astype(part.dtype)

    def pair(p, combine, last=False):
        b = 2 * p
        tiles = [None, None]
        stat_tile = jnp.zeros((GROUP, lanes), jnp.float32)
        for i in range(2):
            vcopy(b + i).wait()
            kcopy(b + i + 2).wait()
            if combine and i == 0:
                for copy in stat_copies(p - LAG) + part_copies(p - LAG):
                    copy.wait_recv()
            tiles[i] = [values(b + i, i, g) for g in range(groups)]
            stat_tile = scores(b + i + 2, i, stat_tile)
            if combine:
                if i == 0:
                    scale = scales(p - LAG)
                together(p - LAG, i, scale)
            if i:
                stat[p + 1] = stat_tile
                for h in range(groups // 2):
                    store(p, *tiles, h)

            @pl.when(b + i + SLOTS < batch - 2)
            def _():
                vcopy(b + i + SLOTS).start()

            for g in range(groups):

                @pl.when(jnp.logical_and(b + i + SLOTS >= batch - 2, b + i + SLOTS < batch))
                def _():
                    vpiece(b + i + SLOTS, g).start()

            @pl.when(b + i + 2 + SLOTS < batch)
            def _():
                kcopy(b + i + 2 + SLOTS).start()

    def send_pair(p):
        for copy in stat_copies(p) + part_copies(p):
            copy.start()

    def sent(p):
        for copy in stat_copies(p) + part_copies(p):
            copy.wait_send()

    qcopy.wait()
    stat_tile = jnp.zeros((GROUP, lanes), jnp.float32)
    for b in range(2):
        kcopy(b).wait()
        stat_tile = scores(b, b, stat_tile)
        kcopy(b + SLOTS).start()
        vcopy(b + SLOTS - 2).start()
    stat[0] = stat_tile

    pair(0, False)
    pl.semaphore_wait(barrier, len(PEERS))

    def step(p, combine):
        @pl.when(p >= 3)
        def _():
            sent(p - 3)

        send_pair(p - 1)
        pair(p, combine)

    @pl.loop(1, LAG)
    def _(p):
        step(p, False)

    @pl.loop(LAG, pairs - 1)
    def _(p):
        step(p, True)

    p = pairs - 1
    sent(p - 3)
    send_pair(p - 1)
    sent(p - 2)
    for copy in stat_copies(p):
        copy.start()
    even = []
    for g in range(groups):
        vpiece(batch - 2, g).wait()
        even.append(values(batch - 2, 0, g))
    for h in range(groups // 2):
        odd_tiles = {}
        for g in (2 * h, 2 * h + 1):
            vpiece(batch - 1, g).wait()
            odd_tiles[g] = values(batch - 1, 1, g)
        store(p, even, odd_tiles, h)
        for copy in half_copies(p, h):
            copy.start()

    @pl.loop(p - LAG, p)
    def _(c):
        for copy in stat_copies(c) + part_copies(c):
            copy.wait_recv()
        scale = scales(c)
        for h in range(groups // 2):
            together(c, h, scale)

    for copy in stat_copies(p):
        copy.wait_recv()
    scale = scales(p)
    for h in range(groups // 2):
        for copy in half_copies(p, h):
            copy.wait_recv()
        together(p, h, scale)

    sent(p - 1)
    for copy in stat_copies(p) + half_copies(p, 0) + half_copies(p, 1):
        copy.wait_send()


def solution(mesh):
    def step(q, k, v):
        batch, tokens, heads, head = k.shape
        pairs = batch // 2
        k, v = (jnp.transpose(x, (0, 2, 3, 1)).reshape(batch, heads * head, tokens) for x in (k, v))
        q = pltpu.with_memory_space_constraint(q, pltpu.HBM)
        n, groups = len(PEERS), heads // GROUP
        block = pltpu.VMEM((SLOTS, heads * head, tokens), jnp.bfloat16)
        return pl.pallas_call(
            functools.partial(attend, pairs, heads, head),
            out_shape=jax.ShapeDtypeStruct(q.shape, q.dtype),
            in_specs=[pl.BlockSpec(memory_space=pltpu.HBM)] * 3,
            out_specs=pl.BlockSpec(memory_space=pltpu.VMEM),
            scratch_shapes=[
                pltpu.VMEM(q.shape, q.dtype),
                block,
                block,
                pltpu.VMEM((2, heads, tokens), jnp.float32),
                pltpu.VMEM((pairs, heads, 2 * head), jnp.bfloat16),
                pltpu.VMEM((pairs, GROUP, 2 * head), jnp.float32),
                pltpu.VMEM((n, pairs, heads, 2 * head), jnp.bfloat16),
                pltpu.VMEM((n, pairs, GROUP, 2 * head), jnp.float32),
                pltpu.SemaphoreType.DMA,
                pltpu.SemaphoreType.DMA((SLOTS,)),
                pltpu.SemaphoreType.DMA((SLOTS,)),
                pltpu.SemaphoreType.DMA((2, groups)),
                pltpu.SemaphoreType.DMA((2, n, 3)),
                pltpu.SemaphoreType.DMA((pairs, n, 3)),
            ],
            compiler_params=pltpu.CompilerParams(collective_id=0, has_side_effects=True, vmem_limit_bytes=48 * 2**20),
        )(q, k, v)

    return jax.shard_map(
        step,
        mesh=mesh,
        in_specs=(P("dp", None, None), P("dp", "sp", None, None), P("dp", "sp", None, None)),
        out_specs=P("dp", None, None),
        check_vma=False,
    )
```

```python
import functools

import jax
import jax.numpy as jnp
from jax import lax
from jax.experimental import pallas as pl
from jax.experimental.pallas import tpu as pltpu
from jax.sharding import PartitionSpec as P

MESH = pl.DeviceIdType.MESH
SLOTS = 6
LAG = 4
RING = 2 * LAG + 1
GROUP = 8
PEERS = [(x, y, c) for x in (1, 0) for y in (1, 0) for c in (1, 0)][:-1]


def add(terms):
    return functools.reduce(jnp.add, terms)


def attend(pairs, heads, head, q_hbm, k_hbm, v_hbm, out_ref, q_ref, kbuf, vbuf, raw, weights, part, stat, parts, stats, qsem, ksem, vsem, lsem, send, recv):
    batch, groups, lanes = 2 * pairs, heads // GROUP, 2 * head
    rows = GROUP * head
    me = lax.axis_index("sp")
    mx, my, mc = me // 4, (me // 2) % 2, me % 2
    devices = [((mx + x) % 2) * 4 + ((my + y) % 2) * 2 + (mc + c) % 2 for x, y, c in PEERS]

    def kcopy(b):
        return pltpu.make_async_copy(k_hbm.at[b], kbuf.at[b % SLOTS], ksem.at[b % SLOTS])

    def vcopy(b):
        return pltpu.make_async_copy(v_hbm.at[b], vbuf.at[b % SLOTS], vsem.at[b % SLOTS])

    def vpiece(b, g):
        piece = pl.ds(g * rows, rows)
        return pltpu.make_async_copy(v_hbm.at[b, piece], vbuf.at[b % SLOTS, piece], lsem.at[b % 2, g])

    qcopy = pltpu.make_async_copy(q_hbm, q_ref, qsem)
    qcopy.start()
    for b in range(4):
        kcopy(b).start(priority=1)
    for b in range(SLOTS - 2):
        vcopy(b).start(priority=1)
        if b + 4 < SLOTS:
            kcopy(b + 4).start(priority=1)

    barrier = pltpu.get_barrier_semaphore()
    for device in devices:
        pl.semaphore_signal(barrier, inc=1, device_id={"sp": device}, device_id_type=MESH)

    lane = lax.broadcasted_iota(jnp.int32, (GROUP, lanes), 1)
    row = lax.broadcasted_iota(jnp.int32, (GROUP, lanes), 0)
    own = [row == 2 * j + lane // head for j in range(GROUP // 2)]
    odd = (lane // head) == row % 2

    def score(b, i, g):
        query = q_ref[b, g * GROUP : (g + 1) * GROUP, :].astype(jnp.float32)
        query = jnp.concatenate([query, query], 1)
        spread = jnp.concatenate([jnp.where(o, query, 0.0) for o in own], 1).astype(jnp.bfloat16)
        keys = kbuf[b % SLOTS, g * rows : (g + 1) * rows, :]
        raw[i, g * GROUP : (g + 1) * GROUP, :] = jnp.dot(spread, keys, preferred_element_type=jnp.float32)

    def soften():
        stat_tile = jnp.zeros((GROUP, lanes), jnp.float32)
        for i in range(2):
            for g in range(groups):
                s = raw[i, g * GROUP : (g + 1) * GROUP, :] * head**-0.5
                high = jnp.max(s, 1, keepdims=True)
                w = jnp.exp(s - high)
                weights[i, g * GROUP : (g + 1) * GROUP, :] = w.astype(weights.dtype)
                total = jnp.sum(w, 1, keepdims=True)
                at = g * 4 + i * 2
                stat_tile = jnp.where(lane == at, high, jnp.where(lane == at + 1, total, stat_tile))
        return stat_tile

    def values(b, i, g):
        w = weights[i, g * GROUP : (g + 1) * GROUP, :].astype(jnp.bfloat16)
        block = vbuf[b % SLOTS, g * rows : (g + 1) * rows, :]
        seen = lax.dot_general(w, block, (((1,), (1,)), ((), ())), preferred_element_type=jnp.float32)
        return add(jnp.where(o, seen[:, j * lanes : (j + 1) * lanes], 0.0) for j, o in enumerate(own))

    def copies(src, dst, kind, p):
        return [
            pltpu.make_async_remote_copy(
                src_ref=src,
                dst_ref=dst.at[r],
                send_sem=send.at[kind, p % 2],
                recv_sem=recv.at[kind, p % RING],
                device_id={"sp": device},
                device_id_type=MESH,
            )
            for r, device in enumerate(devices)
        ]

    def arrived(dst, kind, p):
        return pltpu.make_async_remote_copy(
            src_ref=dst,
            dst_ref=dst,
            send_sem=send.at[kind, p % 2],
            recv_sem=recv.at[kind, p % RING],
            device_id={"sp": devices[0]},
            device_id_type=MESH,
        )

    def half(h):
        return pl.ds(h * 2 * GROUP, 2 * GROUP)

    def send_stat(p):
        for copy in copies(stat.at[p], stats.at[:, p], 0, p):
            copy.start()

    def send_part(p):
        for copy in copies(part.at[p], parts.at[:, p], 1, p):
            copy.start()

    def send_half(p, h):
        for copy in copies(part.at[p, half(h)], parts.at[:, p, half(h)], 1 + h, p):
            copy.start()

    def scales(p):
        each = [stat[p]] + [stats[r, p] for r in range(len(PEERS))]
        high = functools.reduce(jnp.maximum, each)
        scale = [jnp.exp(e - high) for e in each]
        total = add(pltpu.roll(e, lanes - 1, 1) * s for e, s in zip(each, scale))
        scale = [s / total for s in scale]
        return [[jnp.where(odd, s[:, 4 * g + 2 : 4 * g + 3], s[:, 4 * g : 4 * g + 1]) for s in scale] for g in range(groups)]

    def together(p, h, scale):
        piece = slice(h * 2 * GROUP, (h + 1) * 2 * GROUP)
        tiles = [t.astype(jnp.float32) for t in [part[p, piece, :]] + [parts[r, p, piece, :] for r in range(len(PEERS))]]
        result = [[], []]
        for i in range(2):
            both = add(t[i * GROUP : (i + 1) * GROUP] * s for t, s in zip(tiles, scale[2 * h + i]))
            swapped = pltpu.roll(both, head, 1)
            result[0].append(jnp.where(row % 2 == 0, swapped, both)[:, :head])
            result[1].append(jnp.where(row % 2 == 0, both, swapped)[:, :head])
        for i in range(2):
            out_ref[2 * p + i, piece, :] = jnp.concatenate(result[i], 0).astype(out_ref.dtype)

    def store(p, even, odd_tiles, h):
        tile = jnp.concatenate([pltpu.roll(even[g], head, 1) + odd_tiles[g] for g in (2 * h, 2 * h + 1)], 0)
        part[p, h * 2 * GROUP : (h + 1) * 2 * GROUP, :] = tile.astype(part.dtype)

    def attended(p):
        return [[values(2 * p + i, i, g) for g in range(groups)] for i in range(2)]

    def pair(p, combine):
        b = 2 * p
        for i in range(2):
            vcopy(b + i).wait()
            kcopy(b + i + 4).wait()
        if combine:
            received(p - LAG)
        tiles = attended(p)
        stat[p + 1] = soften()
        for i in range(2):
            for g in range(groups):
                score(b + i + 4, i, g)
        if combine:
            scale = scales(p - LAG)
            for h in range(groups // 2):
                together(p - LAG, h, scale)
        for h in range(groups // 2):
            store(p, *tiles, h)
        refill(b)

    def refill(b):
        for i in range(2):
            v, k = b + i + SLOTS, b + i + 4 + SLOTS

            @pl.when(v < batch - 2)
            def _():
                vcopy(v).start(priority=1)

            @pl.when(jnp.logical_and(v >= batch - 2, v < batch))
            def _():
                for g in range(groups):
                    vpiece(v, g).start(priority=1)

            @pl.when(k < batch)
            def _():
                kcopy(k).start(priority=1)

    def received(p):
        arrived(stats.at[:, p], 0, p).wait_recv()
        arrived(parts.at[:, p], 1, p).wait_recv()

    def send_pair(p):
        send_stat(p)
        send_part(p)

    def sent(p):
        arrived(stats.at[:, p], 0, p).wait_send()
        arrived(parts.at[:, p], 1, p).wait_send()

    qcopy.wait()
    for i in range(2):
        kcopy(i).wait()
    for i in range(2):
        for g in range(groups):
            score(i, i, g)
    for i in range(2):
        kcopy(i + SLOTS).start(priority=1)
        kcopy(i + 2).wait()
    stat[0] = soften()
    for i in range(2):
        for g in range(groups):
            score(i + 2, i, g)
    for i in range(2):
        kcopy(i + 2 + SLOTS).start(priority=1)
        vcopy(i + SLOTS - 2).start(priority=1)

    pair(0, False)
    pl.semaphore_wait(barrier, len(PEERS))

    def step(p, combine):
        @pl.when(p >= 3)
        def _():
            sent(p - 3)

        send_pair(p - 1)
        pair(p, combine)

    @pl.loop(1, LAG)
    def _(p):
        step(p, False)

    @pl.loop(LAG, pairs - 2)
    def _(p):
        step(p, True)

    p = pairs - 2
    sent(p - 3)
    send_pair(p - 1)
    for i in range(2):
        vcopy(2 * p + i).wait()
    received(p - LAG)
    tiles = attended(p)
    stat[p + 1] = soften()
    scale = scales(p - LAG)
    for h in range(groups // 2):
        together(p - LAG, h, scale)
        store(p, *tiles, h)

    p = pairs - 1
    sent(p - 3)
    send_pair(p - 1)
    sent(p - 2)
    send_stat(p)
    even = []
    for g in range(groups):
        vpiece(batch - 2, g).wait()
        even.append(values(batch - 2, 0, g))
    for h in range(groups // 2):
        odd_tiles = {}
        for g in (2 * h, 2 * h + 1):
            vpiece(batch - 1, g).wait()
            odd_tiles[g] = values(batch - 1, 1, g)
        store(p, even, odd_tiles, h)
        send_half(p, h)

    @pl.loop(p - LAG, p)
    def _(c):
        received(c)
        scale = scales(c)
        for h in range(groups // 2):
            together(c, h, scale)

    arrived(stats.at[:, p], 0, p).wait_recv()
    scale = scales(p)
    for h in range(groups // 2):
        arrived(parts.at[:, p, half(h)], 1 + h, p).wait_recv()
        together(p, h, scale)

    sent(p - 1)
    arrived(stats.at[:, p], 0, p).wait_send()
    for h in range(groups // 2):
        arrived(parts.at[:, p, half(h)], 1 + h, p).wait_send()


def solution(mesh):
    def step(q, k, v):
        batch, tokens, heads, head = k.shape
        pairs = batch // 2
        k, v = (jnp.transpose(x, (0, 2, 3, 1)).reshape(batch, heads * head, tokens) for x in (k, v))
        q = pltpu.with_memory_space_constraint(q, pltpu.HBM)
        n, groups = len(PEERS), heads // GROUP
        block = pltpu.VMEM((SLOTS, heads * head, tokens), jnp.bfloat16)
        return pl.pallas_call(
            functools.partial(attend, pairs, heads, head),
            out_shape=jax.ShapeDtypeStruct(q.shape, q.dtype),
            in_specs=[pl.BlockSpec(memory_space=pltpu.HBM)] * 3,
            out_specs=pl.BlockSpec(memory_space=pltpu.VMEM),
            scratch_shapes=[
                pltpu.VMEM(q.shape, q.dtype),
                block,
                block,
                pltpu.VMEM((2, heads, tokens), jnp.float32),
                pltpu.VMEM((2, heads, tokens), jnp.float32),
                pltpu.VMEM((pairs, heads, 2 * head), jnp.bfloat16),
                pltpu.VMEM((pairs, GROUP, 2 * head), jnp.float32),
                pltpu.VMEM((n, pairs, heads, 2 * head), jnp.bfloat16),
                pltpu.VMEM((n, pairs, GROUP, 2 * head), jnp.float32),
                pltpu.SemaphoreType.DMA,
                pltpu.SemaphoreType.DMA((SLOTS,)),
                pltpu.SemaphoreType.DMA((SLOTS,)),
                pltpu.SemaphoreType.DMA((2, groups)),
                pltpu.SemaphoreType.DMA((3, 2)),
                pltpu.SemaphoreType.DMA((3, RING)),
            ],
            compiler_params=pltpu.CompilerParams(collective_id=0, has_side_effects=True, vmem_limit_bytes=48 * 2**20),
        )(q, k, v)

    return jax.shard_map(
        step,
        mesh=mesh,
        in_specs=(P("dp", None, None), P("dp", "sp", None, None), P("dp", "sp", None, None)),
        out_specs=P("dp", None, None),
        check_vma=False,
    )
```

```python
import functools

import jax
import jax.numpy as jnp
from jax import lax
from jax.experimental import pallas as pl
from jax.experimental.pallas import tpu as pltpu
from jax.sharding import PartitionSpec as P

MESH = pl.DeviceIdType.MESH
SLOTS = 6
LAG = 3
RING = 2 * LAG + 1
GROUP = 8
PEERS = [(x, y, c) for x in (1, 0) for y in (1, 0) for c in (1, 0)][:-1]


def add(terms):
    return functools.reduce(jnp.add, terms)


def attend(pairs, heads, head, q_hbm, k_hbm, v_hbm, out_ref, q_ref, kbuf, vbuf, raw, weights, part, stat, parts, stats, qsem, ksem, vsem, send, recv):
    batch, groups, lanes = 2 * pairs, heads // GROUP, 2 * head
    rows = GROUP * head
    me = lax.axis_index("sp")
    mx, my, mc = me // 4, (me // 2) % 2, me % 2
    devices = [((mx + x) % 2) * 4 + ((my + y) % 2) * 2 + (mc + c) % 2 for x, y, c in PEERS]

    def kcopy(b):
        return pltpu.make_async_copy(k_hbm.at[b], kbuf.at[b % SLOTS], ksem.at[b % SLOTS])

    def vcopy(b):
        return pltpu.make_async_copy(v_hbm.at[b], vbuf.at[b % SLOTS], vsem.at[b % SLOTS])

    qcopy = pltpu.make_async_copy(q_hbm, q_ref, qsem)
    qcopy.start()
    for b in range(4):
        kcopy(b).start(priority=1)
    for b in range(SLOTS - 2):
        vcopy(b).start(priority=1)
        if b + 4 < SLOTS:
            kcopy(b + 4).start(priority=1)

    barrier = pltpu.get_barrier_semaphore()
    for device in devices:
        pl.semaphore_signal(barrier, inc=1, device_id={"sp": device}, device_id_type=MESH)

    lane = lax.broadcasted_iota(jnp.int32, (GROUP, lanes), 1)
    row = lax.broadcasted_iota(jnp.int32, (GROUP, lanes), 0)
    own = [row == 2 * j + lane // head for j in range(GROUP // 2)]
    odd = (lane // head) == row % 2

    def score(b, i, g):
        query = q_ref[b, g * GROUP : (g + 1) * GROUP, :].astype(jnp.float32)
        query = jnp.concatenate([query, query], 1)
        spread = jnp.concatenate([jnp.where(o, query, 0.0) for o in own], 1).astype(jnp.bfloat16)
        keys = kbuf[b % SLOTS, g * rows : (g + 1) * rows, :]
        raw[i, g * GROUP : (g + 1) * GROUP, :] = jnp.dot(spread, keys, preferred_element_type=jnp.float32)

    def soften(i, stat_tile):
        for g in range(groups):
            s = raw[i, g * GROUP : (g + 1) * GROUP, :] * head**-0.5
            high = jnp.max(s, 1, keepdims=True)
            w = jnp.exp(s - high)
            weights[i, g * GROUP : (g + 1) * GROUP, :] = w
            total = jnp.sum(w, 1, keepdims=True)
            at = g * 4 + i * 2
            stat_tile = jnp.where(lane == at, high, jnp.where(lane == at + 1, total, stat_tile))
        return stat_tile

    nothing = jnp.zeros((GROUP, lanes), jnp.float32)

    def values(b, i, g):
        w = weights[i, g * GROUP : (g + 1) * GROUP, :].astype(jnp.bfloat16)
        block = vbuf[b % SLOTS, g * rows : (g + 1) * rows, :]
        seen = lax.dot_general(w, block, (((1,), (1,)), ((), ())), preferred_element_type=jnp.float32)
        return add(jnp.where(o, seen[:, j * lanes : (j + 1) * lanes], 0.0) for j, o in enumerate(own))

    def copies(src, dst, kind, p):
        return [
            pltpu.make_async_remote_copy(
                src_ref=src,
                dst_ref=dst.at[r],
                send_sem=send.at[kind * 2 + (p % 2 if kind < 2 else 0)],
                recv_sem=recv.at[kind * RING + (p % RING if kind < 2 else 0)],
                device_id={"sp": device},
                device_id_type=MESH,
            )
            for r, device in enumerate(devices)
        ]

    def arrived(dst, kind, p):
        return pltpu.make_async_remote_copy(
            src_ref=dst,
            dst_ref=dst,
            send_sem=send.at[kind * 2 + (p % 2 if kind < 2 else 0)],
            recv_sem=recv.at[kind * RING + (p % RING if kind < 2 else 0)],
            device_id={"sp": devices[0]},
            device_id_type=MESH,
        )

    def half(h):
        return pl.ds(h * 2 * GROUP, 2 * GROUP)

    def send_stat(p):
        for copy in copies(stat.at[p], stats.at[:, p], 0, p):
            copy.start()

    def send_part(p):
        for copy in copies(part.at[p], parts.at[:, p], 1, p):
            copy.start()

    def send_half(p, h):
        for copy in copies(part.at[p, half(h)], parts.at[:, p, half(h)], 1 + h, p):
            copy.start()

    def scales(p):
        each = [stat[p]] + [stats[r, p] for r in range(len(PEERS))]
        high = functools.reduce(jnp.maximum, each)
        scale = [jnp.exp(e - high) for e in each]
        total = add(pltpu.roll(e, lanes - 1, 1) * s for e, s in zip(each, scale))
        scale = [s / total for s in scale]
        return [[jnp.where(odd, s[:, 4 * g + 2 : 4 * g + 3], s[:, 4 * g : 4 * g + 1]) for s in scale] for g in range(groups)]

    def together(p, h, scale):
        piece = slice(h * 2 * GROUP, (h + 1) * 2 * GROUP)
        tiles = [t.astype(jnp.float32) for t in [part[p, piece, :]] + [parts[r, p, piece, :] for r in range(len(PEERS))]]
        result = [[], []]
        for i in range(2):
            both = add(t[i * GROUP : (i + 1) * GROUP] * s for t, s in zip(tiles, scale[2 * h + i]))
            swapped = pltpu.roll(both, head, 1)
            result[0].append(jnp.where(row % 2 == 0, swapped, both)[:, :head])
            result[1].append(jnp.where(row % 2 == 0, both, swapped)[:, :head])
        for i in range(2):
            out_ref[2 * p + i, piece, :] = jnp.concatenate(result[i], 0).astype(out_ref.dtype)

    def store(p, even, odd_tiles, h):
        tile = jnp.concatenate([pltpu.roll(even[g], head, 1) + odd_tiles[g] for g in (2 * h, 2 * h + 1)], 0)
        part[p, h * 2 * GROUP : (h + 1) * 2 * GROUP, :] = tile.astype(part.dtype)

    def attended(b, i):
        return [values(b, i, g) for g in range(groups)]

    def pair(p, combine):
        b = 2 * p
        for i in range(2):
            vcopy(b + i).wait()
            kcopy(b + i + 4).wait()
        if combine:
            received(p - LAG)
        tiles = [attended(b + i, i) for i in range(2)]
        stat[p + 1] = soften(1, soften(0, nothing))
        for i in range(2):
            for g in range(groups):
                score(b + i + 4, i, g)
        if combine:
            scale = scales(p - LAG)
            for h in range(groups // 2):
                together(p - LAG, h, scale)
        for h in range(groups // 2):
            store(p, *tiles, h)
        refill(b)

    def refill(b):
        for i in range(2):
            v, k = b + i + SLOTS, b + i + 4 + SLOTS

            @pl.when(v < batch)
            def _():
                vcopy(v).start(priority=1)

            @pl.when(k < batch)
            def _():
                kcopy(k).start(priority=1)

    def received(p):
        arrived(stats.at[:, p], 0, p).wait_recv()
        arrived(parts.at[:, p], 1, p).wait_recv()

    def send_pair(p):
        send_stat(p)
        send_part(p)

    def sent(p):
        arrived(stats.at[:, p], 0, p).wait_send()
        arrived(parts.at[:, p], 1, p).wait_send()

    qcopy.wait()
    for i in range(2):
        kcopy(i).wait()
    for i in range(2):
        for g in range(groups):
            score(i, i, g)
    for i in range(2):
        kcopy(i + SLOTS).start(priority=1)
        kcopy(i + 2).wait()
    stat[0] = soften(1, soften(0, nothing))
    for i in range(2):
        for g in range(groups):
            score(i + 2, i, g)
    for i in range(2):
        kcopy(i + 2 + SLOTS).start(priority=1)
        vcopy(i + SLOTS - 2).start(priority=1)

    pair(0, False)
    pl.semaphore_wait(barrier, len(PEERS))

    def step(p, combine):
        @pl.when(p >= 3)
        def _():
            sent(p - 3)

        send_pair(p - 1)
        pair(p, combine)

    @pl.loop(1, LAG)
    def _(p):
        step(p, False)

    @pl.loop(LAG, pairs - 3)
    def _(p):
        step(p, True)

    for p in range(pairs - 3, pairs - 1):
        sent(p - 3)
        send_pair(p - 1)
        received(p - LAG)
        tiles, stat_tile = [], nothing
        for i in range(2):
            b = 2 * p + i
            vcopy(b).wait()
            if b + 4 < batch:
                kcopy(b + 4).wait()
            tiles.append(attended(b, i))
            stat_tile = soften(i, stat_tile)
            if b + 4 < batch:
                for g in range(groups):
                    score(b + 4, i, g)
        stat[p + 1] = stat_tile
        for h in range(groups // 2):
            store(p, *tiles, h)

    p = pairs - 1
    sent(p - 3)
    send_pair(p - 1)
    sent(p - 2)
    send_stat(p)
    vcopy(batch - 2).wait()
    even = attended(batch - 2, 0)
    vcopy(batch - 1).wait()
    for h in range(groups // 2):
        odd_tiles = {g: values(batch - 1, 1, g) for g in (2 * h, 2 * h + 1)}
        store(p, even, odd_tiles, h)
        send_half(p, h)

    def combine(c):
        scale = scales(c)
        for h in range(groups // 2):
            together(c, h, scale)

    pl.loop(p - 2 - LAG, p - LAG)(combine)

    @pl.loop(p - LAG, p)
    def _(c):
        received(c)
        combine(c)

    arrived(stats.at[:, p], 0, p).wait_recv()
    scale = scales(p)
    for h in range(groups // 2):
        arrived(parts.at[:, p, half(h)], 1 + h, p).wait_recv()
        together(p, h, scale)

    sent(p - 1)
    arrived(stats.at[:, p], 0, p).wait_send()
    for h in range(groups // 2):
        arrived(parts.at[:, p, half(h)], 1 + h, p).wait_send()


def solution(mesh):
    def step(q, k, v):
        batch, tokens, heads, head = k.shape
        pairs = batch // 2
        k, v = (jnp.transpose(x, (0, 2, 3, 1)).reshape(batch, heads * head, tokens) for x in (k, v))
        q = pltpu.with_memory_space_constraint(q, pltpu.HBM)
        n, groups = len(PEERS), heads // GROUP
        block = pltpu.VMEM((SLOTS, heads * head, tokens), jnp.bfloat16)
        return pl.pallas_call(
            functools.partial(attend, pairs, heads, head),
            out_shape=jax.ShapeDtypeStruct(q.shape, q.dtype),
            in_specs=[pl.BlockSpec(memory_space=pltpu.HBM)] * 3,
            out_specs=pl.BlockSpec(memory_space=pltpu.VMEM),
            scratch_shapes=[
                pltpu.VMEM(q.shape, q.dtype),
                block,
                block,
                pltpu.VMEM((2, heads, tokens), jnp.float32),
                pltpu.VMEM((2, heads, tokens), jnp.float32),
                pltpu.VMEM((pairs, heads, 2 * head), jnp.bfloat16),
                pltpu.VMEM((pairs, GROUP, 2 * head), jnp.float32),
                pltpu.VMEM((n, pairs, heads, 2 * head), jnp.bfloat16),
                pltpu.VMEM((n, pairs, GROUP, 2 * head), jnp.float32),
                pltpu.SemaphoreType.DMA,
                pltpu.SemaphoreType.DMA((SLOTS,)),
                pltpu.SemaphoreType.DMA((SLOTS,)),
                pltpu.SemaphoreType.DMA((5,)),
                pltpu.SemaphoreType.DMA((2 * RING + 1,)),
            ],
            compiler_params=pltpu.CompilerParams(collective_id=0, has_side_effects=True, vmem_limit_bytes=48 * 2**20),
        )(q, k, v)

    return jax.shard_map(
        step,
        mesh=mesh,
        in_specs=(P("dp", None, None), P("dp", "sp", None, None), P("dp", "sp", None, None)),
        out_specs=P("dp", None, None),
        check_vma=False,
    )
```

```python
import functools

import jax
import jax.numpy as jnp
from jax import lax
from jax.experimental import pallas as pl
from jax.experimental.pallas import tpu as pltpu
from jax.sharding import PartitionSpec as P

MESH = pl.DeviceIdType.MESH
SLOTS = 6
LAG = 4
RING = 2 * LAG
GROUP = 8
SHARED = (3,)
TAIL = 4
PEERS = [(x, y, c) for x in (1, 0) for y in (1, 0) for c in (1, 0)][:-1]


def add(terms):
    return functools.reduce(jnp.add, terms)


def attend(pairs, heads, head, q_hbm, k_hbm, v_hbm, out_ref, q_ref, kbuf, vbuf, raw, weights, part, stat, parts, stats, qsem, ksem, vsem, send, recv):
    batch, groups, lanes, tokens = 2 * pairs, heads // GROUP, 2 * head, kbuf.shape[2]
    rows = GROUP * head
    me = lax.axis_index("sp")
    mx, my, mc = me // 4, (me // 2) % 2, me % 2
    devices = [((mx + x) % 2) * 4 + ((my + y) % 2) * 2 + (mc + c) % 2 for x, y, c in PEERS]

    def kcopy(b):
        return pltpu.make_async_copy(k_hbm.at[b], kbuf.at[b % SLOTS], ksem.at[b % SLOTS])

    def vcopy(b):
        return pltpu.make_async_copy(v_hbm.at[b], vbuf.at[b % SLOTS], vsem.at[b % SLOTS])

    qcopy = pltpu.make_async_copy(q_hbm, q_ref, qsem)
    qcopy.start()
    for b in range(4):
        kcopy(b).start(priority=1)
    for b in range(SLOTS - 2):
        vcopy(b).start(priority=1)
        if b + 4 < SLOTS:
            kcopy(b + 4).start(priority=1)

    barrier = pltpu.get_barrier_semaphore()
    for device in devices:
        pl.semaphore_signal(barrier, inc=1, device_id={"sp": device}, device_id_type=MESH)

    lane = lax.broadcasted_iota(jnp.int32, (GROUP, lanes), 1)
    row = lax.broadcasted_iota(jnp.int32, (GROUP, lanes), 0)
    own = [row == 2 * j + lane // head for j in range(GROUP // 2)]
    odd = (lane // head) == row % 2

    def score(b, i, g):
        query = q_ref[b, g * GROUP : (g + 1) * GROUP, :].astype(jnp.float32)
        query = jnp.concatenate([query, query], 1)
        spread = jnp.concatenate([jnp.where(o, query, 0.0) for o in own], 1).astype(jnp.bfloat16)
        keys = kbuf[b % SLOTS, g * rows : (g + 1) * rows, :]
        raw[i, g * GROUP : (g + 1) * GROUP, :] = jnp.dot(spread, keys, preferred_element_type=jnp.float32)

    def soften(i, stat_tile, place):
        for g in range(groups):
            s = raw[i, g * GROUP : (g + 1) * GROUP, :] * head**-0.5
            high = jnp.max(s, 1, keepdims=True)
            w = jnp.exp(s - high)
            weights[i, g * GROUP : (g + 1) * GROUP, :] = w
            total = jnp.sum(w, 1, keepdims=True)
            at = place + g * 4 + i * 2
            stat_tile = jnp.where(lane == at, high, jnp.where(lane == at + 1, total, stat_tile))
        return stat_tile

    def place_of(p):
        return p % 2 * 4 * groups

    def tile_of(p):
        return jnp.where(p % 2 == 1, stat[p // 2], 0.0)

    def values(b, i, g):
        w = weights[i, g * GROUP : (g + 1) * GROUP, :].astype(jnp.bfloat16)
        block = vbuf[b % SLOTS, g * rows : (g + 1) * rows, :]
        seen = lax.dot_general(w, block, (((1,), (1,)), ((), ())), preferred_element_type=jnp.float32)
        return add(jnp.where(o, seen[:, j * lanes : (j + 1) * lanes], 0.0) for j, o in enumerate(own))

    def values_by_lanes(b, i, g):
        w = weights[i, g * GROUP : (g + 1) * GROUP, :].astype(jnp.bfloat16).astype(jnp.float32)
        seen = []
        for h in range(GROUP):
            at = g * rows + h * head
            block = vbuf[b % SLOTS, at : at + head, :].astype(jnp.float32) * w[h : h + 1]
            block = add(block[:, j * lanes : (j + 1) * lanes] for j in range(tokens // lanes))
            seen.append(jnp.sum(block.T, 0, keepdims=True))
        seen = jnp.concatenate(seen, 0)
        return jnp.where(lane // head == row % 2, jnp.concatenate([seen, seen], 1), 0.0)

    def copies(src, dst, sent, got):
        return [
            pltpu.make_async_remote_copy(
                src_ref=src,
                dst_ref=dst.at[r],
                send_sem=send.at[sent],
                recv_sem=recv.at[got],
                device_id={"sp": device},
                device_id_type=MESH,
            )
            for r, device in enumerate(devices)
        ]

    def all_of(dst, sent, got):
        return pltpu.make_async_remote_copy(
            src_ref=dst,
            dst_ref=dst,
            send_sem=send.at[sent],
            recv_sem=recv.at[got],
            device_id={"sp": devices[0]},
            device_id_type=MESH,
        )

    def half(h):
        return pl.ds(h * 2 * GROUP, 2 * GROUP)

    end = pairs - 1

    def part_message(p):
        return part.at[p], parts.at[:, p], p % 2, p % RING

    def stat_message(p):
        m = p // 2
        return stat.at[m], stats.at[:, m], 2 + m % 2, RING + m % (RING // 2)

    def last_message(h):
        return part.at[end, half(h)], parts.at[:, end, half(h)], 4 + h, RING + RING // 2 + h

    def start(message):
        for copy in copies(*message):
            copy.start()

    def wait_sent(message):
        all_of(*message[1:]).wait_send()

    def wait_got(message):
        all_of(*message[1:]).wait_recv()

    def send_pair(p):
        @pl.when(p >= 2)
        def _():
            wait_sent(part_message(p - 2))

        start(part_message(p))

        def two():
            @pl.when(p >= 4)
            def _():
                wait_sent(stat_message(p - 4))

            start(stat_message(p))

        when_even(p, two)

    def got(p):
        wait_got(part_message(p))
        when_even(p, lambda: wait_got(stat_message(p)))

    def when_even(p, do):
        if isinstance(p, int):
            if p % 2 == 0:
                do()
        else:
            pl.when(p % 2 == 0)(do)

    def scales(p):
        each = [stat[p // 2]] + [stats[r, p // 2] for r in range(len(PEERS))]
        high = functools.reduce(jnp.maximum, each)
        scale = [jnp.exp(e - high) for e in each]
        total = add(pltpu.roll(e, lanes - 1, 1) * s for e, s in zip(each, scale))
        scale = [pltpu.roll(s / total, (lanes - place_of(p)) % lanes, 1) for s in scale]
        return [[jnp.where(odd, s[:, 4 * g + 2 : 4 * g + 3], s[:, 4 * g : 4 * g + 1]) for s in scale] for g in range(groups)]

    def together(p, h, scale):
        piece = slice(h * 2 * GROUP, (h + 1) * 2 * GROUP)
        tiles = [t.astype(jnp.float32) for t in [part[p, piece, :]] + [parts[r, p, piece, :] for r in range(len(PEERS))]]
        result = [[], []]
        for i in range(2):
            both = add(t[i * GROUP : (i + 1) * GROUP] * s for t, s in zip(tiles, scale[2 * h + i]))
            swapped = pltpu.roll(both, head, 1)
            result[0].append(jnp.where(row % 2 == 0, swapped, both)[:, :head])
            result[1].append(jnp.where(row % 2 == 0, both, swapped)[:, :head])
        for i in range(2):
            out_ref[2 * p + i, piece, :] = jnp.concatenate(result[i], 0).astype(out_ref.dtype)

    def store(p, even, odd_tiles, h):
        tile = jnp.concatenate([pltpu.roll(even[g], head, 1) + odd_tiles[g] for g in (2 * h, 2 * h + 1)], 0)
        part[p, h * 2 * GROUP : (h + 1) * 2 * GROUP, :] = tile.astype(part.dtype)

    def attended(b, i, shared=False):
        return [(values_by_lanes if shared and g in SHARED else values)(b, i, g) for g in range(groups)]

    def pair(p, combine):
        b = 2 * p
        for i in range(2):
            vcopy(b + i).wait()
            kcopy(b + i + 4).wait()
        if combine:
            got(p - LAG)
        tiles = [attended(b + i, i) for i in range(2)]
        place = place_of(p + 1)
        stat[(p + 1) // 2] = soften(1, soften(0, tile_of(p + 1), place), place)
        for i in range(2):
            for g in range(groups):
                score(b + i + 4, i, g)
        if combine:
            scale = scales(p - LAG)
            for h in range(groups // 2):
                together(p - LAG, h, scale)
        for h in range(groups // 2):
            store(p, *tiles, h)
        for i in range(2):
            refill(b + i)

    def refill(b):
        @pl.when(b + SLOTS < batch)
        def _():
            vcopy(b + SLOTS).start(priority=1)

        @pl.when(b + 4 + SLOTS < batch)
        def _():
            kcopy(b + 4 + SLOTS).start(priority=1)

    qcopy.wait()
    for i in range(2):
        kcopy(i).wait()
    for i in range(2):
        for g in range(groups):
            score(i, i, g)
    for i in range(2):
        kcopy(i + SLOTS).start(priority=1)
        kcopy(i + 2).wait()
    stat[0] = soften(1, soften(0, jnp.zeros((GROUP, lanes), jnp.float32), 0), 0)
    for i in range(2):
        for g in range(groups):
            score(i + 2, i, g)
    for i in range(2):
        kcopy(i + 2 + SLOTS).start(priority=1)
        vcopy(i + SLOTS - 2).start(priority=1)

    pair(0, False)
    pl.semaphore_wait(barrier, len(PEERS))

    def step(p, combine):
        send_pair(p - 1)
        pair(p, combine)

    @pl.loop(1, LAG)
    def _(p):
        step(p, False)

    @pl.loop(LAG, pairs - TAIL)
    def _(p):
        step(p, True)

    for p in range(pairs - TAIL, pairs - 1):
        send_pair(p - 1)
        got(p - LAG)
        tiles, stat_tile = [], tile_of(p + 1)
        for i in range(2):
            b = 2 * p + i
            vcopy(b).wait()
            if b + 4 < batch:
                kcopy(b + 4).wait()
            tiles.append(attended(b, i, b + 4 >= batch))
            stat_tile = soften(i, stat_tile, place_of(p + 1))
            if b + 4 < batch:
                for g in range(groups):
                    score(b + 4, i, g)
            refill(b)
        stat[(p + 1) // 2] = stat_tile
        for h in range(groups // 2):
            store(p, *tiles, h)

    send_pair(end - 1)
    vcopy(batch - 2).wait()
    even = attended(batch - 2, 0, True)
    vcopy(batch - 1).wait()
    for h in range(groups // 2):
        odd_tiles = {g: (values_by_lanes if g in SHARED else values)(batch - 1, 1, g) for g in (2 * h, 2 * h + 1)}
        store(end, even, odd_tiles, h)
        start(last_message(h))

    def combine(c):
        scale = scales(c)
        for h in range(groups // 2):
            together(c, h, scale)

    pl.loop(pairs - TAIL - LAG, end - LAG)(combine)

    @pl.loop(end - LAG, end)
    def _(c):
        got(c)
        combine(c)

    scale = scales(end)
    for h in range(groups // 2):
        wait_got(last_message(h))
        together(end, h, scale)

    for p in (end - 2, end - 1):
        wait_sent(part_message(p))
    for p in (end - 3, end - 1):
        wait_sent(stat_message(p))
    for h in range(groups // 2):
        wait_sent(last_message(h))


def solution(mesh):
    def step(q, k, v):
        batch, tokens, heads, head = k.shape
        pairs = batch // 2
        k, v = (jnp.transpose(x, (0, 2, 3, 1)).reshape(batch, heads * head, tokens) for x in (k, v))
        q = pltpu.with_memory_space_constraint(q, pltpu.HBM)
        n, groups = len(PEERS), heads // GROUP
        block = pltpu.VMEM((SLOTS, heads * head, tokens), jnp.bfloat16)
        return pl.pallas_call(
            functools.partial(attend, pairs, heads, head),
            out_shape=jax.ShapeDtypeStruct(q.shape, q.dtype),
            in_specs=[pl.BlockSpec(memory_space=pltpu.HBM)] * 3,
            out_specs=pl.BlockSpec(memory_space=pltpu.VMEM),
            scratch_shapes=[
                pltpu.VMEM(q.shape, q.dtype),
                block,
                block,
                pltpu.VMEM((2, heads, tokens), jnp.float32),
                pltpu.VMEM((2, heads, tokens), jnp.float32),
                pltpu.VMEM((pairs, heads, 2 * head), jnp.bfloat16),
                pltpu.VMEM((pairs // 2, GROUP, 2 * head), jnp.float32),
                pltpu.VMEM((n, pairs, heads, 2 * head), jnp.bfloat16),
                pltpu.VMEM((n, pairs // 2, GROUP, 2 * head), jnp.float32),
                pltpu.SemaphoreType.DMA,
                pltpu.SemaphoreType.DMA((SLOTS,)),
                pltpu.SemaphoreType.DMA((SLOTS,)),
                pltpu.SemaphoreType.DMA((4 + groups // 2,)),
                pltpu.SemaphoreType.DMA((RING + RING // 2 + groups // 2,)),
            ],
            compiler_params=pltpu.CompilerParams(collective_id=0, has_side_effects=True, vmem_limit_bytes=48 * 2**20),
        )(q, k, v)

    return jax.shard_map(
        step,
        mesh=mesh,
        in_specs=(P("dp", None, None), P("dp", "sp", None, None), P("dp", "sp", None, None)),
        out_specs=P("dp", None, None),
        check_vma=False,
    )
```

```python
import functools

import jax
import jax.numpy as jnp
from jax import lax
from jax.experimental import pallas as pl
from jax.experimental.pallas import tpu as pltpu
from jax.sharding import PartitionSpec as P

MESH = pl.DeviceIdType.MESH
SLOTS = 6
LAG = 4
RING = 2 * LAG
GROUP = 8
SHARED = (1, 3)
TAIL = 4
PEERS = [(x, y, c) for x in (1, 0) for y in (1, 0) for c in (1, 0)][:-1]


def add(terms):
    return functools.reduce(jnp.add, terms)


def attend(pairs, heads, head, q_hbm, k_hbm, v_hbm, out_ref, q_ref, kbuf, vbuf, raw, weights, part, stat, parts, stats, qsem, ksem, vsem, send, recv):
    batch, groups, lanes, tokens = 2 * pairs, heads // GROUP, 2 * head, kbuf.shape[2]
    rows = GROUP * head
    me = lax.axis_index("sp")
    mx, my, mc = me // 4, (me // 2) % 2, me % 2
    devices = [((mx + x) % 2) * 4 + ((my + y) % 2) * 2 + (mc + c) % 2 for x, y, c in PEERS]

    def kcopy(b):
        return pltpu.make_async_copy(k_hbm.at[b], kbuf.at[b % SLOTS], ksem.at[b % SLOTS])

    def vcopy(b):
        return pltpu.make_async_copy(v_hbm.at[b], vbuf.at[b % SLOTS], vsem.at[b % SLOTS])

    qcopy = pltpu.make_async_copy(q_hbm, q_ref, qsem)
    qcopy.start()
    for b in range(4):
        kcopy(b).start(priority=1)
    for b in range(SLOTS - 2):
        vcopy(b).start(priority=1)
        if b + 4 < SLOTS:
            kcopy(b + 4).start(priority=1)

    barrier = pltpu.get_barrier_semaphore()
    for device in devices:
        pl.semaphore_signal(barrier, inc=1, device_id={"sp": device}, device_id_type=MESH)

    lane = lax.broadcasted_iota(jnp.int32, (GROUP, lanes), 1)
    row = lax.broadcasted_iota(jnp.int32, (GROUP, lanes), 0)
    own = [row == 2 * j + lane // head for j in range(GROUP // 2)]
    odd = (lane // head) == row % 2

    def score(b, i, g):
        query = q_ref[b, g * GROUP : (g + 1) * GROUP, :].astype(jnp.float32)
        query = jnp.concatenate([query, query], 1)
        spread = jnp.concatenate([jnp.where(o, query, 0.0) for o in own], 1).astype(jnp.bfloat16)
        keys = kbuf[b % SLOTS, g * rows : (g + 1) * rows, :]
        raw[i, g * GROUP : (g + 1) * GROUP, :] = jnp.dot(spread, keys, preferred_element_type=jnp.float32)

    def soften(i, stat_tile, place, to=0):
        for g in range(groups):
            s = raw[i, g * GROUP : (g + 1) * GROUP, :] * head**-0.5
            high = jnp.max(s, 1, keepdims=True)
            w = jnp.exp(s - high)
            weights[to + i, g * GROUP : (g + 1) * GROUP, :] = w
            total = jnp.sum(w, 1, keepdims=True)
            at = place + g * 4 + i * 2
            stat_tile = jnp.where(lane == at, high, jnp.where(lane == at + 1, total, stat_tile))
        return stat_tile

    def place_of(p):
        return p % 2 * 4 * groups

    def tile_of(p):
        return jnp.where(p % 2 == 1, stat[p // 2], 0.0)

    def values(b, i, g):
        w = weights[i, g * GROUP : (g + 1) * GROUP, :].astype(jnp.bfloat16)
        block = vbuf[b % SLOTS, g * rows : (g + 1) * rows, :]
        seen = lax.dot_general(w, block, (((1,), (1,)), ((), ())), preferred_element_type=jnp.float32)
        return add(jnp.where(o, seen[:, j * lanes : (j + 1) * lanes], 0.0) for j, o in enumerate(own))

    def values_by_lanes(b, i, g):
        w = weights[i, g * GROUP : (g + 1) * GROUP, :].astype(jnp.bfloat16).astype(jnp.float32)
        seen = []
        for h in range(GROUP):
            at = g * rows + h * head
            block = vbuf[b % SLOTS, at : at + head, :].astype(jnp.float32) * w[h : h + 1]
            block = add(block[:, j * lanes : (j + 1) * lanes] for j in range(tokens // lanes))
            seen.append(jnp.sum(block.T, 0, keepdims=True))
        seen = jnp.concatenate(seen, 0)
        return jnp.where(lane // head == row % 2, jnp.concatenate([seen, seen], 1), 0.0)

    def copies(src, dst, sent, got):
        return [
            pltpu.make_async_remote_copy(
                src_ref=src,
                dst_ref=dst.at[r],
                send_sem=send.at[sent],
                recv_sem=recv.at[got],
                device_id={"sp": device},
                device_id_type=MESH,
            )
            for r, device in enumerate(devices)
        ]

    def all_of(dst, sent, got):
        return pltpu.make_async_remote_copy(
            src_ref=dst,
            dst_ref=dst,
            send_sem=send.at[sent],
            recv_sem=recv.at[got],
            device_id={"sp": devices[0]},
            device_id_type=MESH,
        )

    def half(h):
        return pl.ds(h * 2 * GROUP, 2 * GROUP)

    end = pairs - 1

    def part_message(p):
        return part.at[p], parts.at[:, p], p % 2, p % RING

    def stat_message(p):
        m = p // 2
        return stat.at[m], stats.at[:, m], 2 + m % 2, RING + m % (RING // 2)

    def last_message(h):
        return part.at[end, half(h)], parts.at[:, end, half(h)], 4 + h, RING + RING // 2 + h

    def start(message):
        for copy in copies(*message):
            copy.start()

    def wait_sent(message):
        all_of(*message[1:]).wait_send()

    def wait_got(message):
        all_of(*message[1:]).wait_recv()

    def send_part(p):
        @pl.when(p >= 2)
        def _():
            wait_sent(part_message(p - 2))

        start(part_message(p))

    def send_stat(p):
        @pl.when(p >= 4)
        def _():
            wait_sent(stat_message(p - 4))

        start(stat_message(p))

    def send_pair(p):
        send_part(p)
        when_even(p, lambda: send_stat(p))

    def got(p):
        wait_got(part_message(p))
        when_even(p, lambda: wait_got(stat_message(p)))

    def when_even(p, do):
        if isinstance(p, int):
            if p % 2 == 0:
                do()
        else:
            pl.when(p % 2 == 0)(do)

    def scales(p):
        each = [stat[p // 2]] + [stats[r, p // 2] for r in range(len(PEERS))]
        high = functools.reduce(jnp.maximum, each)
        scale = [jnp.exp(e - high) for e in each]
        total = add(pltpu.roll(e, lanes - 1, 1) * s for e, s in zip(each, scale))
        scale = [pltpu.roll(s / total, (lanes - place_of(p)) % lanes, 1) for s in scale]
        return [[jnp.where(odd, s[:, 4 * g + 2 : 4 * g + 3], s[:, 4 * g : 4 * g + 1]) for s in scale] for g in range(groups)]

    def together(p, h, scale):
        piece = slice(h * 2 * GROUP, (h + 1) * 2 * GROUP)
        tiles = [t.astype(jnp.float32) for t in [part[p, piece, :]] + [parts[r, p, piece, :] for r in range(len(PEERS))]]
        result = [[], []]
        for i in range(2):
            both = add(t[i * GROUP : (i + 1) * GROUP] * s for t, s in zip(tiles, scale[2 * h + i]))
            swapped = pltpu.roll(both, head, 1)
            result[0].append(jnp.where(row % 2 == 0, swapped, both)[:, :head])
            result[1].append(jnp.where(row % 2 == 0, both, swapped)[:, :head])
        for i in range(2):
            out_ref[2 * p + i, piece, :] = jnp.concatenate(result[i], 0).astype(out_ref.dtype)

    def store(p, even, odd_tiles, h):
        tile = jnp.concatenate([pltpu.roll(even[g], head, 1) + odd_tiles[g] for g in (2 * h, 2 * h + 1)], 0)
        part[p, h * 2 * GROUP : (h + 1) * 2 * GROUP, :] = tile.astype(part.dtype)

    def attended(b, i, shared=False):
        return [(values_by_lanes if shared and g in SHARED else values)(b, i, g) for g in range(groups)]

    def pair(p, combine):
        b = 2 * p
        for i in range(2):
            vcopy(b + i).wait()
            kcopy(b + i + 4).wait()
        if combine:
            got(p - LAG)
        tiles = [attended(b + i, i) for i in range(2)]
        place = place_of(p + 1)
        stat[(p + 1) // 2] = soften(1, soften(0, tile_of(p + 1), place), place)
        for i in range(2):
            for g in range(groups):
                score(b + i + 4, i, g)
        if combine:
            scale = scales(p - LAG)
            for h in range(groups // 2):
                together(p - LAG, h, scale)
        for h in range(groups // 2):
            store(p, *tiles, h)
        for i in range(2):
            refill(b + i)

    def refill(b):
        @pl.when(b + SLOTS < batch)
        def _():
            vcopy(b + SLOTS).start(priority=1)

        @pl.when(b + 4 + SLOTS < batch)
        def _():
            kcopy(b + 4 + SLOTS).start(priority=1)

    qcopy.wait()
    for i in range(2):
        kcopy(i).wait()
    for i in range(2):
        for g in range(groups):
            score(i, i, g)
    for i in range(2):
        kcopy(i + SLOTS).start(priority=1)
        kcopy(i + 2).wait()
    stat[0] = soften(1, soften(0, jnp.zeros((GROUP, lanes), jnp.float32), 0), 0)
    for i in range(2):
        for g in range(groups):
            score(i + 2, i, g)
    for i in range(2):
        kcopy(i + 2 + SLOTS).start(priority=1)
        vcopy(i + SLOTS - 2).start(priority=1)

    pair(0, False)
    pl.semaphore_wait(barrier, len(PEERS))

    def step(p, combine):
        send_pair(p - 1)
        pair(p, combine)

    @pl.loop(1, LAG)
    def _(p):
        step(p, False)

    @pl.loop(LAG, pairs - TAIL)
    def _(p):
        step(p, True)

    for p in range(pairs - TAIL, pairs - 1):
        send_pair(p - 1)
        got(p - LAG)
        tiles, stat_tile, place = [], tile_of(p + 1), place_of(p + 1)
        if p == end - 1:
            stat[p // 2] = soften(1, soften(0, stat_tile, place, 2), place, 2)
            send_stat(p)
        for i in range(2):
            b = 2 * p + i
            vcopy(b).wait()
            if b + 4 < batch:
                kcopy(b + 4).wait()
            tiles.append(attended(b, i, True))
            if p < end - 1:
                stat_tile = soften(i, stat_tile, place)
            if b + 4 < batch:
                for g in range(groups):
                    score(b + 4, i, g)
            refill(b)
        if p < end - 1:
            stat[(p + 1) // 2] = stat_tile
        for h in range(groups // 2):
            store(p, *tiles, h)

    send_part(end - 1)
    vcopy(batch - 2).wait()
    even = attended(batch - 2, 2, True)
    vcopy(batch - 1).wait()
    for h in range(groups // 2):
        odd_tiles = {g: (values_by_lanes if g in SHARED else values)(batch - 1, 3, g) for g in (2 * h, 2 * h + 1)}
        store(end, even, odd_tiles, h)
        start(last_message(h))

    def combine(c):
        scale = scales(c)
        for h in range(groups // 2):
            together(c, h, scale)

    pl.loop(pairs - TAIL - LAG, end - LAG)(combine)

    @pl.loop(end - LAG, end)
    def _(c):
        got(c)
        combine(c)

    scale = scales(end)
    for h in range(groups // 2):
        wait_got(last_message(h))
        together(end, h, scale)

    for p in (end - 2, end - 1):
        wait_sent(part_message(p))
    for p in (end - 3, end - 1):
        wait_sent(stat_message(p))
    for h in range(groups // 2):
        wait_sent(last_message(h))


def solution(mesh):
    def step(q, k, v):
        batch, tokens, heads, head = k.shape
        pairs = batch // 2
        k, v = (jnp.transpose(x, (0, 2, 3, 1)).reshape(batch, heads * head, tokens) for x in (k, v))
        q = pltpu.with_memory_space_constraint(q, pltpu.HBM)
        n, groups = len(PEERS), heads // GROUP
        block = pltpu.VMEM((SLOTS, heads * head, tokens), jnp.bfloat16)
        return pl.pallas_call(
            functools.partial(attend, pairs, heads, head),
            out_shape=jax.ShapeDtypeStruct(q.shape, q.dtype),
            in_specs=[pl.BlockSpec(memory_space=pltpu.HBM)] * 3,
            out_specs=pl.BlockSpec(memory_space=pltpu.VMEM),
            scratch_shapes=[
                pltpu.VMEM(q.shape, q.dtype),
                block,
                block,
                pltpu.VMEM((2, heads, tokens), jnp.float32),
                pltpu.VMEM((4, heads, tokens), jnp.float32),
                pltpu.VMEM((pairs, heads, 2 * head), jnp.bfloat16),
                pltpu.VMEM((pairs // 2, GROUP, 2 * head), jnp.float32),
                pltpu.VMEM((n, pairs, heads, 2 * head), jnp.bfloat16),
                pltpu.VMEM((n, pairs // 2, GROUP, 2 * head), jnp.float32),
                pltpu.SemaphoreType.DMA,
                pltpu.SemaphoreType.DMA((SLOTS,)),
                pltpu.SemaphoreType.DMA((SLOTS,)),
                pltpu.SemaphoreType.DMA((4 + groups // 2,)),
                pltpu.SemaphoreType.DMA((RING + RING // 2 + groups // 2,)),
            ],
            compiler_params=pltpu.CompilerParams(collective_id=0, has_side_effects=True, vmem_limit_bytes=48 * 2**20),
        )(q, k, v)

    return jax.shard_map(
        step,
        mesh=mesh,
        in_specs=(P("dp", None, None), P("dp", "sp", None, None), P("dp", "sp", None, None)),
        out_specs=P("dp", None, None),
        check_vma=False,
    )
```

```python
import functools

import jax
import jax.numpy as jnp
from jax import lax
from jax.experimental import pallas as pl
from jax.experimental.pallas import tpu as pltpu
from jax.sharding import PartitionSpec as P

MESH = pl.DeviceIdType.MESH
SLOTS = 6
LAG = 4
RING = 2 * LAG
GROUP = 8
SHARED = (1, 3)
TAIL = 4
PEERS = [(1, 1, 0), (1, 1, 1), (1, 0, 0), (0, 1, 0), (1, 0, 1), (0, 1, 1), (0, 0, 1)]


def add(terms):
    return functools.reduce(jnp.add, terms)


def attend(pairs, heads, head, q_hbm, k_hbm, v_hbm, out_ref, q_ref, kbuf, vbuf, raw, weights, part, stat, parts, stats, qsem, ksem, vsem, send, recv):
    batch, groups, lanes, tokens = 2 * pairs, heads // GROUP, 2 * head, kbuf.shape[2]
    rows = GROUP * head
    me = lax.axis_index("sp")
    mx, my, mc = me // 4, (me // 2) % 2, me % 2
    devices = [((mx + x) % 2) * 4 + ((my + y) % 2) * 2 + (mc + c) % 2 for x, y, c in PEERS]

    def kcopy(b):
        return pltpu.make_async_copy(k_hbm.at[b], kbuf.at[b % SLOTS], ksem.at[b % SLOTS])

    def vcopy(b):
        return pltpu.make_async_copy(v_hbm.at[b], vbuf.at[b % SLOTS], vsem.at[b % SLOTS])

    qcopy = pltpu.make_async_copy(q_hbm, q_ref, qsem)
    qcopy.start()
    for b in range(4):
        kcopy(b).start(priority=1)
    for b in range(SLOTS - 2):
        vcopy(b).start(priority=1)
        if b + 4 < SLOTS:
            kcopy(b + 4).start(priority=1)

    barrier = pltpu.get_barrier_semaphore()
    for device in devices:
        pl.semaphore_signal(barrier, inc=1, device_id={"sp": device}, device_id_type=MESH)

    lane = lax.broadcasted_iota(jnp.int32, (GROUP, lanes), 1)
    row = lax.broadcasted_iota(jnp.int32, (GROUP, lanes), 0)
    own = [row == 2 * j + lane // head for j in range(GROUP // 2)]
    odd = (lane // head) == row % 2

    def score(b, i, g):
        query = q_ref[b, g * GROUP : (g + 1) * GROUP, :].astype(jnp.float32)
        query = jnp.concatenate([query, query], 1)
        spread = jnp.concatenate([jnp.where(o, query, 0.0) for o in own], 1).astype(jnp.bfloat16)
        keys = kbuf[b % SLOTS, g * rows : (g + 1) * rows, :]
        raw[i, g * GROUP : (g + 1) * GROUP, :] = jnp.dot(spread, keys, preferred_element_type=jnp.float32)

    def soften(i, stat_tile, place, to=0):
        for g in range(groups):
            s = raw[i, g * GROUP : (g + 1) * GROUP, :] * head**-0.5
            high = jnp.max(s, 1, keepdims=True)
            w = jnp.exp(s - high)
            weights[to + i, g * GROUP : (g + 1) * GROUP, :] = w
            total = jnp.sum(w, 1, keepdims=True)
            at = place + g * 4 + i * 2
            stat_tile = jnp.where(lane == at, high, jnp.where(lane == at + 1, total, stat_tile))
        return stat_tile

    def place_of(p):
        return p % 2 * 4 * groups

    def tile_of(p):
        return jnp.where(p % 2 == 1, stat[p // 2], 0.0)

    def values(b, i, g):
        w = weights[i, g * GROUP : (g + 1) * GROUP, :].astype(jnp.bfloat16)
        block = vbuf[b % SLOTS, g * rows : (g + 1) * rows, :]
        seen = lax.dot_general(w, block, (((1,), (1,)), ((), ())), preferred_element_type=jnp.float32)
        return add(jnp.where(o, seen[:, j * lanes : (j + 1) * lanes], 0.0) for j, o in enumerate(own))

    def values_by_lanes(b, i, g):
        w = weights[i, g * GROUP : (g + 1) * GROUP, :].astype(jnp.bfloat16).astype(jnp.float32)
        seen = []
        for h in range(GROUP):
            at = g * rows + h * head
            block = vbuf[b % SLOTS, at : at + head, :].astype(jnp.float32) * w[h : h + 1]
            block = add(block[:, j * lanes : (j + 1) * lanes] for j in range(tokens // lanes))
            seen.append(jnp.sum(block.T, 0, keepdims=True))
        seen = jnp.concatenate(seen, 0)
        return jnp.where(lane // head == row % 2, jnp.concatenate([seen, seen], 1), 0.0)

    def copies(src, dst, sent, got):
        return [
            pltpu.make_async_remote_copy(
                src_ref=src,
                dst_ref=dst.at[r],
                send_sem=send.at[sent],
                recv_sem=recv.at[got],
                device_id={"sp": device},
                device_id_type=MESH,
            )
            for r, device in enumerate(devices)
        ]

    def all_of(dst, sent, got):
        return pltpu.make_async_remote_copy(
            src_ref=dst,
            dst_ref=dst,
            send_sem=send.at[sent],
            recv_sem=recv.at[got],
            device_id={"sp": devices[0]},
            device_id_type=MESH,
        )

    def half(h):
        return pl.ds(h * 2 * GROUP, 2 * GROUP)

    end = pairs - 1

    def part_message(p):
        return part.at[p], parts.at[:, p], p % 2, p % RING

    def stat_message(p):
        m = p // 2
        return stat.at[m], stats.at[:, m], 2 + m % 2, RING + m % (RING // 2)

    def last_message(h):
        return part.at[end, half(h)], parts.at[:, end, half(h)], 4 + h, RING + RING // 2 + h

    def start(message):
        for copy in copies(*message):
            copy.start()

    def wait_sent(message):
        all_of(*message[1:]).wait_send()

    def wait_got(message):
        all_of(*message[1:]).wait_recv()

    def send_part(p):
        @pl.when(p >= 2)
        def _():
            wait_sent(part_message(p - 2))

        start(part_message(p))

    def send_stat(p):
        @pl.when(p >= 4)
        def _():
            wait_sent(stat_message(p - 4))

        start(stat_message(p))

    def send_pair(p):
        send_part(p)
        when_even(p, lambda: send_stat(p))

    def got(p):
        wait_got(part_message(p))
        when_even(p, lambda: wait_got(stat_message(p)))

    def when_even(p, do):
        if isinstance(p, int):
            if p % 2 == 0:
                do()
        else:
            pl.when(p % 2 == 0)(do)

    def scales(p):
        each = [stat[p // 2]] + [stats[r, p // 2] for r in range(len(PEERS))]
        high = functools.reduce(jnp.maximum, each)
        scale = [jnp.exp(e - high) for e in each]
        total = add(pltpu.roll(e, lanes - 1, 1) * s for e, s in zip(each, scale))
        scale = [pltpu.roll(s / total, (lanes - place_of(p)) % lanes, 1) for s in scale]
        return [[jnp.where(odd, s[:, 4 * g + 2 : 4 * g + 3], s[:, 4 * g : 4 * g + 1]) for s in scale] for g in range(groups)]

    def together(p, h, scale):
        piece = slice(h * 2 * GROUP, (h + 1) * 2 * GROUP)
        tiles = [t.astype(jnp.float32) for t in [part[p, piece, :]] + [parts[r, p, piece, :] for r in range(len(PEERS))]]
        result = [[], []]
        for i in range(2):
            both = add(t[i * GROUP : (i + 1) * GROUP] * s for t, s in zip(tiles, scale[2 * h + i]))
            swapped = pltpu.roll(both, head, 1)
            result[0].append(jnp.where(row % 2 == 0, swapped, both)[:, :head])
            result[1].append(jnp.where(row % 2 == 0, both, swapped)[:, :head])
        for i in range(2):
            out_ref[2 * p + i, piece, :] = jnp.concatenate(result[i], 0).astype(out_ref.dtype)

    def store(p, even, odd_tiles, h):
        tile = jnp.concatenate([pltpu.roll(even[g], head, 1) + odd_tiles[g] for g in (2 * h, 2 * h + 1)], 0)
        part[p, h * 2 * GROUP : (h + 1) * 2 * GROUP, :] = tile.astype(part.dtype)

    def attended(b, i, shared=False):
        return [(values_by_lanes if shared and g in SHARED else values)(b, i, g) for g in range(groups)]

    def pair(p, combine):
        b = 2 * p
        for i in range(2):
            vcopy(b + i).wait()
            kcopy(b + i + 4).wait()
        if combine:
            got(p - LAG)
        tiles = [attended(b + i, i) for i in range(2)]
        place = place_of(p + 1)
        stat[(p + 1) // 2] = soften(1, soften(0, tile_of(p + 1), place), place)
        for i in range(2):
            for g in range(groups):
                score(b + i + 4, i, g)
        if combine:
            scale = scales(p - LAG)
            for h in range(groups // 2):
                together(p - LAG, h, scale)
        for h in range(groups // 2):
            store(p, *tiles, h)
        for i in range(2):
            refill(b + i)

    def refill(b):
        @pl.when(b + SLOTS < batch)
        def _():
            vcopy(b + SLOTS).start(priority=1)

        @pl.when(b + 4 + SLOTS < batch)
        def _():
            kcopy(b + 4 + SLOTS).start(priority=1)

    qcopy.wait()
    for i in range(2):
        kcopy(i).wait()
    for i in range(2):
        for g in range(groups):
            score(i, i, g)
    for i in range(2):
        kcopy(i + SLOTS).start(priority=1)
        kcopy(i + 2).wait()
    stat[0] = soften(1, soften(0, jnp.zeros((GROUP, lanes), jnp.float32), 0), 0)
    for i in range(2):
        for g in range(groups):
            score(i + 2, i, g)
    for i in range(2):
        kcopy(i + 2 + SLOTS).start(priority=1)
        vcopy(i + SLOTS - 2).start(priority=1)

    pair(0, False)
    pl.semaphore_wait(barrier, len(PEERS))

    def step(p, combine):
        send_pair(p - 1)
        pair(p, combine)

    @pl.loop(1, LAG)
    def _(p):
        step(p, False)

    @pl.loop(LAG, pairs - TAIL)
    def _(p):
        step(p, True)

    for p in range(pairs - TAIL, pairs - 1):
        send_pair(p - 1)
        got(p - LAG)
        tiles, stat_tile, place = [], tile_of(p + 1), place_of(p + 1)
        if p == end - 1:
            stat[p // 2] = soften(1, soften(0, stat_tile, place, 2), place, 2)
            send_stat(p)
        for i in range(2):
            b = 2 * p + i
            vcopy(b).wait()
            if b + 4 < batch:
                kcopy(b + 4).wait()
            tiles.append(attended(b, i, True))
            if p < end - 1:
                stat_tile = soften(i, stat_tile, place)
            if b + 4 < batch:
                for g in range(groups):
                    score(b + 4, i, g)
            refill(b)
        if p < end - 1:
            stat[(p + 1) // 2] = stat_tile
        for h in range(groups // 2):
            store(p, *tiles, h)

    send_part(end - 1)
    vcopy(batch - 2).wait()
    even = attended(batch - 2, 2, True)
    vcopy(batch - 1).wait()
    for h in range(groups // 2):
        odd_tiles = {g: (values_by_lanes if g in SHARED else values)(batch - 1, 3, g) for g in (2 * h, 2 * h + 1)}
        store(end, even, odd_tiles, h)
        start(last_message(h))

    def combine(c):
        scale = scales(c)
        for h in range(groups // 2):
            together(c, h, scale)

    pl.loop(pairs - TAIL - LAG, end - LAG)(combine)

    @pl.loop(end - LAG, end)
    def _(c):
        got(c)
        combine(c)

    scale = scales(end)
    for h in range(groups // 2):
        wait_got(last_message(h))
        together(end, h, scale)

    for p in (end - 2, end - 1):
        wait_sent(part_message(p))
    for p in (end - 3, end - 1):
        wait_sent(stat_message(p))
    for h in range(groups // 2):
        wait_sent(last_message(h))


def solution(mesh):
    def step(q, k, v):
        batch, tokens, heads, head = k.shape
        pairs = batch // 2
        k, v = (jnp.transpose(x, (0, 2, 3, 1)).reshape(batch, heads * head, tokens) for x in (k, v))
        q = pltpu.with_memory_space_constraint(q, pltpu.HBM)
        n, groups = len(PEERS), heads // GROUP
        block = pltpu.VMEM((SLOTS, heads * head, tokens), jnp.bfloat16)
        return pl.pallas_call(
            functools.partial(attend, pairs, heads, head),
            out_shape=jax.ShapeDtypeStruct(q.shape, q.dtype),
            in_specs=[pl.BlockSpec(memory_space=pltpu.HBM)] * 3,
            out_specs=pl.BlockSpec(memory_space=pltpu.VMEM),
            scratch_shapes=[
                pltpu.VMEM(q.shape, q.dtype),
                block,
                block,
                pltpu.VMEM((2, heads, tokens), jnp.float32),
                pltpu.VMEM((4, heads, tokens), jnp.float32),
                pltpu.VMEM((pairs, heads, 2 * head), jnp.bfloat16),
                pltpu.VMEM((pairs // 2, GROUP, 2 * head), jnp.float32),
                pltpu.VMEM((n, pairs, heads, 2 * head), jnp.bfloat16),
                pltpu.VMEM((n, pairs // 2, GROUP, 2 * head), jnp.float32),
                pltpu.SemaphoreType.DMA,
                pltpu.SemaphoreType.DMA((SLOTS,)),
                pltpu.SemaphoreType.DMA((SLOTS,)),
                pltpu.SemaphoreType.DMA((4 + groups // 2,)),
                pltpu.SemaphoreType.DMA((RING + RING // 2 + groups // 2,)),
            ],
            compiler_params=pltpu.CompilerParams(collective_id=0, has_side_effects=True, vmem_limit_bytes=48 * 2**20),
        )(q, k, v)

    return jax.shard_map(
        step,
        mesh=mesh,
        in_specs=(P("dp", None, None), P("dp", "sp", None, None), P("dp", "sp", None, None)),
        out_specs=P("dp", None, None),
        check_vma=False,
    )
```
